128 devices in a mesh: runs: 32 (over z, y, core), tp: 4 (over x).
Axes of the slice: x: 4, y: 4, z: 4, core: 2. Of those that a mesh axis runs over, the one named last changes fastest.
Arguments:
- hidden: bfloat16 [16384, 8192], P('runs', 'tp'), may hold values from -6 to 6
- cotangent: bfloat16 [16384, 8192], P('runs', 'tp'), may hold values from -0.059814453 to 0.059814453
- rotation: float32 [8192, 512], P(None, 'tp'), may hold values from -0.0625 to 0.0625
- matching: int32 [128], P('runs'), may hold values from 0 to 127
- mask: int32 [128, 128], P('runs'), may hold values 0 or 1
Outputs:
- intervened: bfloat16 [16384, 8192], P('runs', 'tp')
- grad_rotation: float32 [8192, 512], P('runs', 'tp')
The draws below stay inside these ranges and needn't reach their ends.
All inputs are finite; a program needn't handle non-finite values. No bound on the sum of `mask` on one device may be relied on, other than what follows from the above.
Results may differ from the reference program's by a relative error of at most 0.0045.
Values may be sent and summed in bfloat16 or wider, within the bound.
No kernel may reach another device: no remote copies, remote signals or barrier semaphores. Data moves between devices by JAX's collectives and lax.ppermute only.
A program may use at most 128 MiB of HBM per device.

```python
import math
import jax
import jax.numpy as jnp
import numpy as np
from jax import lax

D = 8192
K = 512
L = 128
RUNS = 128
TOKENS = 16384


def plant(array, key, least, top_value):
    longest = array.shape.index(max(array.shape))
    spots = []
    for shift in (0, 1):
        where = [jax.random.randint(jax.random.fold_in(key, axis), (), 0, length) for axis, length in enumerate(array.shape)]
        where[longest] = (where[longest] + shift) % array.shape[longest]
        spots.append(tuple(where))
    return array.at[spots[0]].set(least).at[spots[1]].set(top_value)


def levels(stream_key, shape, shards, least, high):
    factor_of = 1.0
    for axis_at, shards_of in shards:
        steps = jax.random.uniform(jax.random.fold_in(jax.random.fold_in(stream_key, 6), axis_at), (shards_of,), jnp.float32, least / len(shards), high / len(shards))
        factor_of = factor_of * jnp.repeat(jnp.exp(steps), shape[axis_at] // shards_of).reshape((-1,) + (1,) * (len(shape) - 1 - axis_at))
    return factor_of


def cumulative_ranks(number_of, skew):
    weights = [(1 << 20) // math.isqrt(grade ** skew) + 1 for grade in range(1, number_of + 1)]
    spread = 1 + sum(weights) // (1 << 30)
    return np.cumsum(np.array([max(1, weight // spread) for weight in weights]))


def skewed_ids(stream_key, shape, number_of, lean):
    table = cumulative_ranks(number_of, lean)
    lot = jax.random.randint(jax.random.fold_in(stream_key, 1), shape, 0, int(table[number_of - 1]))
    standing = jnp.searchsorted(jnp.asarray(table, jnp.int32), lot, side="right")
    return jax.random.permutation(jax.random.fold_in(stream_key, 2), number_of)[standing].astype(jnp.int32)


def scatter_about(key, extent, scale, bound, pieces=(), dtype=jnp.bfloat16):
    values = scale * jax.random.normal(key, extent, jnp.float32)
    if pieces:
        values = values * levels(key, extent, pieces, -0.22, 0.18)
    return jnp.clip(values, -bound, bound).astype(dtype)


def setup_inputs(seed: int = 0) -> dict:
    arg_keys = jax.random.split(jax.random.key(seed), 6)
    return {
        "hidden": scatter_about(arg_keys[0], (TOKENS, D), 1.0, 6.0, ((0, 32), (1, 4))),
        "cotangent": scatter_about(arg_keys[1], (TOKENS, D), 0.01, 0.059814453, ((0, 32), (1, 4))),
        "rotation": scatter_about(arg_keys[2], (D, K), D ** -0.5, 0.0625, ((1, 4),), jnp.float32),
        "matching": plant(skewed_ids(arg_keys[3], (RUNS,), RUNS, 2), jax.random.fold_in(arg_keys[3], 3), 0, RUNS - 1).astype(jnp.int32),
        "mask": plant((jax.random.randint(arg_keys[4], (RUNS, L), 0, 2) < 1).astype(jnp.int32), jax.random.fold_in(arg_keys[4], 1), 0, 1),
    }


def reference(hidden, cotangent, rotation, matching, mask):
    high = lax.Precision.HIGHEST
    wide_hidden = hidden.astype(jnp.float32)
    wide_cotangent = cotangent.astype(jnp.float32)
    coords = jnp.dot(wide_hidden, rotation, precision=high).reshape(RUNS, L, K)
    chosen = mask.astype(jnp.float32)[:, :, None]
    update = (chosen * (coords[matching] - coords)).reshape(TOKENS, K)
    intervened = (wide_hidden + jnp.dot(update, rotation.T, precision=high)).astype(jnp.bfloat16)
    pulled = chosen * jnp.dot(wide_cotangent, rotation, precision=high).reshape(RUNS, L, K)
    returned = jax.ops.segment_sum(pulled, matching, num_segments=RUNS)
    net = (returned - pulled).reshape(TOKENS, K)
    grad_rotation = jnp.dot(wide_cotangent.T, update, precision=high) + jnp.dot(wide_hidden.T, net, precision=high)
    return intervened, grad_rotation
```

```python
import jax
import jax.numpy as jnp
from jax import lax
from jax.experimental import pallas as pl
from jax.experimental.pallas import tpu as pltpu
from jax.sharding import PartitionSpec as P


Z, Y, CORES, TP = 4, 4, 2, 4
bf16, f32 = jnp.bfloat16, jnp.float32


def along_runs(dz, dy, dcore):
    return [
        (z * 8 + y * 2 + c, (z + dz) % Z * 8 + (y + dy) % Y * 2 + (c + dcore) % CORES)
        for z in range(Z)
        for y in range(Y)
        for c in range(CORES)
    ]


def along_tp(dx):
    return [(x, (x + dx) % TP) for x in range(TP)]


def shift_tp(value, dx):
    return lax.ppermute(value, "tp", along_tp(dx)) if dx % TP else value


def shift_z(value, dz):
    return lax.ppermute(value, "runs", along_runs(dz, 0, 0)) if dz % Z else value


def shift_y(value, dy):
    return lax.ppermute(value, "runs", along_runs(0, dy, 0)) if dy % Y else value


def swap_cores(value):
    return lax.ppermute(value, "runs", along_runs(0, 0, 1))


def dot(a, b, dims=((1,), (0,))):
    return lax.dot_general(a, b, (dims, ((), ())), preferred_element_type=f32)


def pick_runs(index, mine, other):
    count = mine.shape[0]
    block = mine.shape[1:]

    def body(index_ref, mine_ref, other_ref, *outs):
        for k, out in enumerate(outs):
            for i in range(4):
                at = index_ref[4 * k + i]
                near = lax.rem(at, count)
                out[i] = jnp.where(at < count, mine_ref[near], other_ref[near])

    vmem = pl.BlockSpec(memory_space=pltpu.VMEM)
    return pl.pallas_call(
        body,
        out_shape=[jax.ShapeDtypeStruct((4, *block), mine.dtype)] * 4,
        in_specs=[pl.BlockSpec(memory_space=pltpu.SMEM), vmem, vmem],
        out_specs=[vmem] * 4,
    )(index, mine, other)


def add_runs(target, parts):
    block = parts[0].shape[1:]

    def body(target_ref, *refs):
        ins, (near_ref, far_ref, held) = refs[:4], refs[4:]
        held[...] = jnp.zeros_like(held)
        for k, part in enumerate(ins):
            for i in range(4):
                at = target_ref[4 * k + i]
                held[at] = held[at] + part[i].astype(f32)
        near_ref[...] = held[:16]
        far_ref[...] = held[16:32].astype(bf16)

    vmem = pl.BlockSpec(memory_space=pltpu.VMEM)
    return pl.pallas_call(
        body,
        out_shape=[
            jax.ShapeDtypeStruct((16, *block), f32),
            jax.ShapeDtypeStruct((16, *block), bf16),
        ],
        in_specs=[pl.BlockSpec(memory_space=pltpu.SMEM)] + [vmem] * 4,
        out_specs=[vmem] * 2,
        scratch_shapes=[pltpu.VMEM((33, *block), f32)],
    )(target, *parts)


def per_device(hidden, cotangent, rotation, matching, mask):
    tokens, features = hidden.shape
    local_runs, length = mask.shape
    columns = rotation.shape[1]
    half = features // 2
    x, run_at = lax.axis_index("tp"), lax.axis_index("runs")
    z, y, core = run_at // 8, run_at // 2 % Y, run_at % CORES
    every_match = lax.all_gather(matching, "runs", axis=0, tiled=True)

    blocks = []
    for k in range(1, TP):
        start = (x + k) % TP * features + core * half
        part = lax.dynamic_slice(rotation, (start, 0), (half, columns)).astype(bf16)
        got = shift_tp(part, k)
        also = swap_cores(got)
        blocks.append(
            jnp.concatenate(
                [jnp.where(core == 0, got, also), jnp.where(core == 0, also, got)], axis=0
            )
        )
    own_wide = lax.dynamic_slice(rotation, (x * features, 0), (features, columns))
    own_high = lax.reduce_precision(own_wide, 8, 7)
    own_block, own_low = own_high.astype(bf16), (own_wide - own_high).astype(bf16)

    coords = dot(hidden, own_block) + dot(hidden, own_low)
    pulled = dot(cotangent, own_block) + dot(cotangent, own_low)
    for k in range(1, TP):
        part = jnp.concatenate(
            [dot(hidden, blocks[k - 1]), dot(cotangent, blocks[k - 1])], axis=0
        ).astype(bf16)
        got = shift_tp(part, -k).astype(f32)
        coords, pulled = coords + got[:tokens], pulled + got[tokens:]

    own_runs = run_at * local_runs + jnp.arange(local_runs, dtype=jnp.int32)
    chosen = (mask * (matching != own_runs)[:, None].astype(jnp.int32)).astype(f32)
    chosen = chosen[:, :, None]
    own = coords.reshape(local_runs, length, columns)
    pulled = chosen * pulled.reshape(local_runs, length, columns)

    device_of = every_match // local_runs
    source_z, source_y, source_core = device_of // 8, device_of // 2 % Y, device_of % CORES
    slot = (
        (core + source_core) % CORES * 16
        + (z - source_z) % Z * local_runs
        + every_match % local_runs
    )
    in_row = source_y == y

    def of_device(values, dy):
        at = (z * 8 + (y + dy) % Y * 2 + core) * local_runs
        return lax.dynamic_slice(values, (at,), (local_runs,))

    sent = own.astype(bf16)
    near = jnp.concatenate([shift_z(sent, k) for k in range(Z)], axis=0)
    far = swap_cores(near)
    asked = jnp.concatenate([of_device(slot, k) for k in range(Y)])
    served = pick_runs(asked, near, far)
    my_source_y = matching // local_runs // 2 % Y
    picked = jnp.zeros_like(own)
    for k in range(Y):
        got = shift_y(served[k], k).astype(f32)
        picked = jnp.where((my_source_y == (y - k) % Y)[:, None, None], got, picked)
    update = chosen * (picked - own)

    gone = pulled.astype(bf16)
    parts = [shift_y(gone, k) for k in range(Y)]
    targets = jnp.concatenate(
        [jnp.where(of_device(in_row, -k), of_device(slot, -k), 32) for k in range(Y)]
    )
    kept, passed = add_runs(targets, parts)
    kept = kept + swap_cores(passed).astype(f32)
    returned = kept[:local_runs]
    for k in range(1, Z):
        part = kept[k * local_runs : (k + 1) * local_runs].astype(bf16)
        returned = returned + shift_z(part, -k).astype(f32)
    net = returned - pulled

    both = jnp.concatenate([update, net], axis=0).reshape(2 * tokens, columns).astype(bf16)
    every = jnp.concatenate([shift_tp(both, k) for k in range(TP)], axis=1)
    every_update, every_net = every[:tokens], every[tokens:]
    own_rows = jnp.concatenate([own_block, *blocks], axis=1)
    added = dot(every_update, own_rows, ((1,), (1,)))
    intervened = (hidden.astype(f32) + added).astype(bf16)

    grad = dot(cotangent, every_update, ((0,), (0,))) + dot(hidden, every_net, ((0,), (0,)))
    rows = features // (Y * CORES)
    grad = grad.reshape(Y, CORES, rows, TP * columns)
    kept_rows = lax.dynamic_index_in_dim(grad, core, 1, keepdims=False)
    sent_rows = lax.dynamic_index_in_dim(grad, 1 - core, 1, keepdims=False)
    grad = kept_rows + swap_cores(sent_rows)
    grad = grad.reshape(Y, rows, Z, columns).transpose(2, 0, 1, 3)
    grad = grad.reshape(Z * Y, rows, columns).astype(bf16)
    groups = [[z * 8 + y * 2 + c for z in range(Z) for y in range(Y)] for c in range(CORES)]
    grad = lax.all_to_all(grad, "runs", 0, 0, axis_index_groups=groups, tiled=True)
    grad = jnp.sum(grad.astype(f32), axis=0)
    home = [
        ((z * 8 + y * 2 + c) * TP + x, (x * 8 + y * 2 + c) * TP + (x - z) % TP)
        for z in range(Z)
        for y in range(Y)
        for c in range(CORES)
        for x in range(TP)
    ]
    return intervened, lax.ppermute(grad, ("runs", "tp"), home)


def solution(mesh):
    in_specs = (P("runs", "tp"), P("runs", "tp"), P(None, "tp"), P("runs"), P("runs", None))
    out_specs = (P("runs", "tp"), P("runs", "tp"))
    return jax.shard_map(
        per_device, mesh=mesh, in_specs=in_specs, out_specs=out_specs, check_vma=False
    )
```

```python
import jax
import jax.numpy as jnp
from jax import lax
from jax.experimental import pallas as pl
from jax.experimental.pallas import tpu as pltpu
from jax.sharding import PartitionSpec as P


Z, Y, CORES, TP = 4, 4, 2, 4
bf16, f32 = jnp.bfloat16, jnp.float32
VMEM = pl.BlockSpec(memory_space=pltpu.VMEM)
SMEM = pl.BlockSpec(memory_space=pltpu.SMEM)


def along_runs(dz, dy, dcore):
    return [
        (z * 8 + y * 2 + c, (z + dz) % Z * 8 + (y + dy) % Y * 2 + (c + dcore) % CORES)
        for z in range(Z)
        for y in range(Y)
        for c in range(CORES)
    ]


def along_tp(dx):
    return [(x, (x + dx) % TP) for x in range(TP)]


def shift_tp(value, dx):
    return lax.ppermute(value, "tp", along_tp(dx)) if dx % TP else value


def shift_z(value, dz):
    return lax.ppermute(value, "runs", along_runs(dz, 0, 0)) if dz % Z else value


def shift_y(value, dy):
    return lax.ppermute(value, "runs", along_runs(0, dy, 0)) if dy % Y else value


def swap_cores(value):
    return lax.ppermute(value, "runs", along_runs(0, 0, 1))


def dot(a, b, dims=((1,), (0,))):
    return lax.dot_general(a, b, (dims, ((), ())), preferred_element_type=f32)


def kernel(body, outs, scalars, arrays, flops=0, scratch=()):
    call = pl.pallas_call(
        body,
        out_shape=[jax.ShapeDtypeStruct(shape, dtype) for shape, dtype in outs],
        in_specs=[SMEM] * len(scalars) + [VMEM] * len(arrays),
        out_specs=[VMEM] * len(outs),
        scratch_shapes=list(scratch),
        compiler_params=pltpu.CompilerParams(vmem_limit_bytes=16 << 20),
        cost_estimate=pl.CostEstimate(flops=flops, bytes_accessed=0, transcendentals=0)
        if flops
        else None,
    )
    return call(*scalars, *arrays)


def partial_products(core, hidden, cotangent, near, far):
    tokens, features = hidden.shape
    half, columns = near[0].shape
    count = len(near)

    def body(core_ref, hidden_ref, cotangent_ref, *refs):
        ins, outs = refs[: 2 * count], refs[2 * count :]
        at = pl.multiple_of(core_ref[0] * half, half)
        past = pl.multiple_of((1 - core_ref[0]) * half, half)
        here = jnp.concatenate([value[...] for value in ins[:count]], axis=1)
        there = jnp.concatenate([value[...] for value in ins[count:]], axis=1)
        for i, left in enumerate((hidden_ref, cotangent_ref)):
            total = dot(left[:, pl.ds(at, half)], here) + dot(left[:, pl.ds(past, half)], there)
            for k, out in enumerate(outs):
                out[i * tokens : (i + 1) * tokens] = total[
                    :, k * columns : (k + 1) * columns
                ].astype(bf16)

    return kernel(
        body,
        [((2 * tokens, columns), bf16)] * count,
        [core],
        [hidden, cotangent, *near, *far],
        flops=4 * tokens * features * columns * count,
    )


def summed(coords, pulled, parts, chosen):
    tokens, columns = coords.shape

    def body(coords_ref, pulled_ref, chosen_ref, *refs):
        ins, (own, sent, taken, gone) = refs[: TP - 1], refs[TP - 1 :]
        total, other = coords_ref[...], pulled_ref[...]
        for value in ins:
            total = total + value[:tokens].astype(f32)
            other = other + value[tokens:].astype(f32)
        other = other * chosen_ref[...]
        own[...], sent[...] = total, total.astype(bf16)
        taken[...], gone[...] = other, other.astype(bf16)

    shape = (tokens, columns)
    return kernel(
        body,
        [(shape, f32), (shape, bf16), (shape, f32), (shape, bf16)],
        [],
        [coords, pulled, chosen, *parts],
    )


def pick_runs(index, pieces, length):
    shape = pieces[0].shape
    count = len(pieces) * 4

    def body(index_ref, *refs):
        ins, outs, held = refs[: len(pieces)], refs[len(pieces) : -1], refs[-1]
        for k, piece in enumerate(ins):
            held[k * 4 * length : (k + 1) * 4 * length] = piece[...]
        for k, out in enumerate(outs):
            for i in range(4):
                at = pl.multiple_of(index_ref[4 * k + i] * length, length)
                out[i * length : (i + 1) * length] = held[pl.ds(at, length)]

    return kernel(
        body,
        [(shape, bf16)] * Y,
        [index],
        pieces,
        scratch=[pltpu.VMEM((count * length, shape[1]), bf16)],
    )


def add_runs(target, parts, length):
    columns = parts[0].shape[1]
    half = 16 * length

    def body(target_ref, *refs):
        ins, (near, far, held) = refs[:Y], refs[Y:]
        held[...] = jnp.zeros_like(held)
        for k, part in enumerate(ins):
            for i in range(4):
                at = pl.ds(pl.multiple_of(target_ref[4 * k + i] * length, length), length)
                held[at] = held[at] + part[i * length : (i + 1) * length].astype(f32)
        near[...] = held[:half]
        far[...] = held[half : 2 * half].astype(bf16)

    return kernel(
        body,
        [((half, columns), f32), ((half, columns), bf16)],
        [target],
        parts,
        scratch=[pltpu.VMEM((33 * length, columns), f32)],
    )


def split_returned(near, far):
    rows, columns = near.shape
    each = rows // Z

    def body(near_ref, far_ref, *outs):
        for k, out in enumerate(outs):
            at = slice(k * each, (k + 1) * each)
            out[...] = (near_ref[at] + far_ref[at].astype(f32)).astype(out.dtype)

    shape = (each, columns)
    return kernel(body, [(shape, f32)] + [(shape, bf16)] * (Z - 1), [], [near, far])


def update_and_net(from_row, served, own, chosen, returned, others, taken, length):
    tokens, columns = own.shape

    def body(from_ref, own_ref, chosen_ref, returned_ref, taken_ref, *refs):
        rows, ins, out = refs[:Y], refs[Y:-1], refs[-1]
        for i in range(tokens // length):
            at = slice(i * length, (i + 1) * length)
            source = from_ref[i]
            picked = rows[0][at]
            for k in range(1, Y):
                picked = jnp.where(source == k, rows[k][at], picked)
            out[at] = (chosen_ref[at] * (picked.astype(f32) - own_ref[at])).astype(bf16)
        total = returned_ref[...]
        for value in ins:
            total = total + value[...].astype(f32)
        out[tokens:] = (total - taken_ref[...]).astype(bf16)

    return kernel(
        body,
        [((2 * tokens, columns), bf16)],
        [from_row],
        [own, chosen, returned, taken, *served, *others],
    )[0]


def gradient_rows(core, cotangent, hidden, gathered):
    tokens, features = hidden.shape
    rows = features // (Y * CORES)
    columns = gathered[0].shape[1]

    def body(core_ref, cotangent_ref, hidden_ref, *refs):
        ins, out = refs[:TP], refs[TP]
        update = jnp.concatenate([value[:tokens] for value in ins], axis=1)
        net = jnp.concatenate([value[tokens:] for value in ins], axis=1)
        for y in range(Y):
            at = pl.ds(pl.multiple_of((y * CORES + core_ref[0]) * rows, rows), rows)
            block = dot(cotangent_ref[:, at], update, ((0,), (0,)))
            block = block + dot(hidden_ref[:, at], net, ((0,), (0,)))
            for k in range(TP):
                place = (k * Y + y) * rows
                out[place : place + rows] = block[:, k * columns : (k + 1) * columns]

    return kernel(
        body,
        [((TP * Y * rows, columns), f32)],
        [core],
        [cotangent, hidden, *gathered],
        flops=2 * tokens * features * columns * TP,
    )[0]


def intervention(core, hidden, gathered, own_block, near, far):
    tokens, features = hidden.shape
    half = features // 2

    def body(core_ref, hidden_ref, own_ref, *refs):
        ins, rest, out = refs[:TP], refs[TP:-1], refs[-1]
        update = jnp.concatenate([value[:tokens] for value in ins], axis=1)
        for which, pieces in enumerate((rest[: TP - 1], rest[TP - 1 :])):
            place = core_ref[0] if which == 0 else 1 - core_ref[0]
            at = pl.ds(pl.multiple_of(place * half, half), half)
            rows = jnp.concatenate([own_ref[at]] + [value[...] for value in pieces], axis=1)
            added = dot(update, rows, ((1,), (1,)))
            out[:, at] = (hidden_ref[:, at].astype(f32) + added).astype(bf16)

    return kernel(
        body,
        [((tokens, features), bf16)],
        [core],
        [hidden, own_block, *gathered, *near, *far],
        flops=2 * tokens * features * own_block.shape[1] * TP,
    )[0]


def per_device(hidden, cotangent, rotation, matching, mask):
    tokens, features = hidden.shape
    local_runs, length = mask.shape
    columns = rotation.shape[1]
    half = features // 2
    x, run_at = lax.axis_index("tp"), lax.axis_index("runs")
    z, y, core = run_at // 8, run_at // 2 % Y, run_at % CORES
    this_core, other_core = core[None], 1 - core[None]

    near = []
    for k in range(1, TP):
        start = (x + k) % TP * features + core * half
        part = lax.dynamic_slice(rotation, (start, 0), (half, columns)).astype(bf16)
        near.append(shift_tp(part, k))
    far = [swap_cores(value) for value in near]
    own_wide = lax.dynamic_slice(rotation, (x * features, 0), (features, columns))
    own_high = lax.reduce_precision(own_wide, 8, 7)
    own_block, own_low = own_high.astype(bf16), (own_wide - own_high).astype(bf16)
    coords = dot(hidden, own_block) + dot(hidden, own_low)
    pulled = dot(cotangent, own_block) + dot(cotangent, own_low)

    own_runs = run_at * local_runs + jnp.arange(local_runs, dtype=jnp.int32)
    chosen = (mask * (matching != own_runs)[:, None].astype(jnp.int32)).astype(f32)
    chosen = jnp.broadcast_to(chosen[:, :, None], (local_runs, length, columns))
    chosen = chosen.reshape(tokens, columns)

    column_match = [shift_y(matching, -k) for k in range(Y)]

    def slots(match):
        device = match // local_runs
        return (
            (core + device) % CORES * 16
            + (z - device // 8) % Z * local_runs
            + match % local_runs
        )

    asked = jnp.concatenate([slots(match) for match in column_match])
    targets = jnp.concatenate(
        [
            jnp.where(match // local_runs // 2 % Y == y, slots(match), 32)
            for match in (column_match[-k % Y] for k in range(Y))
        ]
    )
    from_row = (y - matching // local_runs // 2) % Y

    parts = partial_products(this_core, hidden, cotangent, near, far)
    parts = [shift_tp(value, -k) for k, value in enumerate(parts, 1)]
    own, sent, taken, gone = summed(coords, pulled, parts, chosen)

    line = [shift_z(sent, k) for k in range(Z)]
    column = [shift_y(gone, k) for k in range(Y)]
    line, column = lax.optimization_barrier((line, column))
    line = line + [swap_cores(value) for value in line]
    kept, passed = add_runs(targets, column, length)
    kept, *moved = split_returned(kept, swap_cores(passed))

    served = pick_runs(asked, line, length)
    served = [shift_y(value, k) for k, value in enumerate(served)]
    moved = [shift_z(value, -k) for k, value in enumerate(moved, 1)]
    both = update_and_net(from_row, served, own, chosen, kept, moved, taken, length)

    gathered = [shift_tp(both, k) for k in range(TP)]
    intervened = intervention(this_core, hidden, gathered, own_block, near, far)

    rows = features // (Y * CORES)
    away = gradient_rows(other_core, cotangent, hidden, gathered)
    grad = gradient_rows(this_core, cotangent, hidden, gathered) + swap_cores(away)
    grad = grad.astype(bf16).reshape(Z * Y, rows, columns)
    groups = [[z * 8 + y * 2 + c for z in range(Z) for y in range(Y)] for c in range(CORES)]
    grad = lax.all_to_all(grad, "runs", 0, 0, axis_index_groups=groups, tiled=True)
    grad = jnp.sum(grad.astype(f32), axis=0)
    home = [
        ((z * 8 + y * 2 + c) * TP + x, (x * 8 + y * 2 + c) * TP + (x - z) % TP)
        for z in range(Z)
        for y in range(Y)
        for c in range(CORES)
        for x in range(TP)
    ]
    return intervened, lax.ppermute(grad, ("runs", "tp"), home)


def solution(mesh):
    in_specs = (P("runs", "tp"), P("runs", "tp"), P(None, "tp"), P("runs"), P("runs", None))
    out_specs = (P("runs", "tp"), P("runs", "tp"))
    return jax.shard_map(
        per_device, mesh=mesh, in_specs=in_specs, out_specs=out_specs, check_vma=False
    )
```

```python
import jax
import jax.numpy as jnp
from jax import lax
from jax.experimental import pallas as pl
from jax.experimental.pallas import tpu as pltpu
from jax.sharding import PartitionSpec as P


Z, Y, CORES, TP = 4, 4, 2, 4
bf16, f32 = jnp.bfloat16, jnp.float32
ORDER = (1, 3, 2)
STRETCHES = 2
VMEM = pl.BlockSpec(memory_space=pltpu.VMEM)
SMEM = pl.BlockSpec(memory_space=pltpu.SMEM)


def along_runs(dz, dy, dcore):
    return [
        (z * 8 + y * 2 + c, (z + dz) % Z * 8 + (y + dy) % Y * 2 + (c + dcore) % CORES)
        for z in range(Z)
        for y in range(Y)
        for c in range(CORES)
    ]


def along_tp(dx):
    return [(x, (x + dx) % TP) for x in range(TP)]


def shift_tp(value, dx):
    return lax.ppermute(value, "tp", along_tp(dx)) if dx % TP else value


def shift_y(value, dy):
    return lax.ppermute(value, "runs", along_runs(0, dy, 0)) if dy % Y else value


def by_core(value, first, second):
    pairs = along_runs(*first, 0)[0::2] + along_runs(*second, 0)[1::2]
    return lax.ppermute(value, "runs", pairs)


def swap_cores(value):
    return lax.ppermute(value, "runs", along_runs(0, 0, 1))


def ordered(send):
    sent = {k: send(k) for k in ORDER}
    return [sent[k] for k in sorted(sent)]


def dot(a, b, dims=((1,), (0,))):
    return lax.dot_general(a, b, (dims, ((), ())), preferred_element_type=f32)


def kernel(body, outs, scalars, arrays, flops=0, scratch=(), grant=16):
    call = pl.pallas_call(
        body,
        out_shape=[jax.ShapeDtypeStruct(shape, dtype) for shape, dtype in outs],
        in_specs=[SMEM] * len(scalars) + [VMEM] * len(arrays),
        out_specs=[VMEM] * len(outs),
        scratch_shapes=list(scratch),
        compiler_params=pltpu.CompilerParams(vmem_limit_bytes=grant << 20),
        cost_estimate=pl.CostEstimate(flops=flops, bytes_accessed=0, transcendentals=0)
        if flops
        else None,
    )
    return call(*scalars, *arrays)


def stretched(value, length):
    each = length // STRETCHES
    starts = range(0, value.shape[0], length)
    return [
        jnp.concatenate([value[at + part * each : at + (part + 1) * each] for at in starts])
        for part in range(STRETCHES)
    ]


def joined(parts, length):
    each = length // STRETCHES
    starts = range(0, parts[0].shape[0], each)
    return jnp.concatenate([part[at : at + each] for at in starts for part in parts])


def own_products(hidden, cotangent, own, length):
    tokens = hidden.shape[0]
    shape = (tokens // STRETCHES, own.shape[1])

    def body(hidden_ref, cotangent_ref, own_ref, rounded, *outs):
        high = own_ref[...].astype(bf16)
        low = (own_ref[...] - high.astype(f32)).astype(bf16)
        rounded[...] = high
        both = jnp.concatenate([high, low], axis=1)
        for i, left in enumerate((hidden_ref, cotangent_ref)):
            total = dot(left[...], both)
            total = total[:, : shape[1]] + total[:, shape[1] :]
            for part, pieces in enumerate(stretched(total, length)):
                outs[i * STRETCHES + part][...] = pieces

    outs = kernel(
        body,
        [(own.shape, bf16)] + [(shape, f32)] * 2 * STRETCHES,
        [],
        [hidden, cotangent, own],
        flops=8 * tokens * own.shape[0] * own.shape[1],
    )
    return outs[0], list(outs[1 : 1 + STRETCHES]), list(outs[1 + STRETCHES :])


def partial_products(core, hidden, cotangent, near, far, length):
    tokens, features = hidden.shape
    half, columns = near[0].shape
    count = len(near)

    rows = 2 * tokens // STRETCHES

    def body(core_ref, hidden_ref, cotangent_ref, *refs):
        ins, outs = refs[: 2 * count], refs[2 * count :]
        at = pl.multiple_of(core_ref[0] * half, half)
        past = pl.multiple_of((1 - core_ref[0]) * half, half)
        here = jnp.concatenate([value[...] for value in ins[:count]], axis=1)
        there = jnp.concatenate([value[...] for value in ins[count:]], axis=1)
        for i, left in enumerate((hidden_ref, cotangent_ref)):
            total = dot(left[:, pl.ds(at, half)], here) + dot(left[:, pl.ds(past, half)], there)
            for part, pieces in enumerate(stretched(total.astype(bf16), length)):
                for k in range(count):
                    place = slice(i * rows // 2, (i + 1) * rows // 2)
                    outs[part * count + k][place] = pieces[:, k * columns : (k + 1) * columns]

    outs = kernel(
        body,
        [((rows, columns), bf16)] * count * STRETCHES,
        [core],
        [hidden, cotangent, *near, *far],
        flops=4 * tokens * features * columns * count,
    )
    return [outs[part * count : (part + 1) * count] for part in range(STRETCHES)]


def summed(core, coords, pulled, parts, chosen):
    tokens, columns = coords.shape

    def body(core_ref, coords_ref, pulled_ref, chosen_ref, *refs):
        ins, (own, taken, keep, give) = refs[: TP - 1], refs[TP - 1 :]
        total, other = coords_ref[...], pulled_ref[...]
        for value in ins:
            total = total + value[:tokens].astype(f32)
            other = other + value[tokens:].astype(f32)
        other = other * chosen_ref[...]
        own[...], taken[...] = total, other
        first = core_ref[0] == 0
        keep[...] = jnp.where(first, total, other).astype(bf16)
        give[...] = jnp.where(first, other, total).astype(bf16)

    shape = (tokens, columns)
    return kernel(
        body,
        [(shape, f32), (shape, f32), (shape, bf16), (shape, bf16)],
        [core],
        [coords, pulled, chosen, *parts],
    )


def copied(value):
    def body(value_ref, out):
        out[...] = value_ref[...]

    return kernel(body, [(value.shape, value.dtype)], [], [value])[0]


def both_cores(core, keep, got):
    tokens, columns = keep.shape

    def body(core_ref, keep_ref, got_ref, out):
        out[pl.ds(pl.multiple_of(core_ref[0] * tokens, tokens), tokens)] = keep_ref[...]
        out[pl.ds(pl.multiple_of((1 - core_ref[0]) * tokens, tokens), tokens)] = got_ref[...]

    return kernel(body, [((2 * tokens, columns), bf16)], [core], [keep, got])[0]


def route_runs(core, index, parts, length):
    shape = parts[0].shape
    each = shape[0] // length
    slots = each * Z

    def body(core_ref, index_ref, *refs):
        ins, outs, (wide, packed, held) = refs[:Z], refs[Z : 2 * Z], refs[2 * Z :]

        @pl.when(core_ref[0] == 0)
        def _():
            for k, part in enumerate(ins):
                packed[k * shape[0] : (k + 1) * shape[0]] = part[...]
            for k, out in enumerate(outs):
                for i in range(each):
                    at = pl.multiple_of(index_ref[each * k + i] * length, length)
                    out[i * length : (i + 1) * length] = packed[pl.ds(at, length)]
            wide[...] = jnp.zeros_like(wide)

        @pl.when(core_ref[0] != 0)
        def _():
            held[...] = jnp.zeros_like(held)
            for k, part in enumerate(ins):
                for i in range(each):
                    at = pl.multiple_of(index_ref[each * k + i] * length, length)
                    at = pl.ds(at, length)
                    held[at] = held[at] + part[i * length : (i + 1) * length].astype(f32)
            for k, out in enumerate(outs):
                out[...] = held[k * shape[0] : (k + 1) * shape[0]].astype(bf16)
            wide[...] = held[: shape[0]]

    return kernel(
        body,
        [(shape, bf16)] * Z + [(shape, f32)],
        [core, index],
        parts,
        scratch=[
            pltpu.VMEM((slots * length, shape[1]), bf16),
            pltpu.VMEM(((slots + 1) * length, shape[1]), f32),
        ],
    )


def finished_runs(core, from_row, wide, parts, length):
    rows, columns = wide.shape
    half = rows // 2

    def body(core_ref, from_ref, wide_ref, *refs):
        ins, (keep, give) = refs[:Z], refs[Z:]

        @pl.when(core_ref[0] == 0)
        def _():
            for i in range(rows // length):
                at = slice(i * length, (i + 1) * length)
                source = from_ref[i]
                picked = ins[0][at]
                for k in range(1, Y):
                    picked = jnp.where(source == k, ins[k][at], picked)
                out = keep if i * length < half else give
                out[i * length % half : i * length % half + length] = picked.astype(f32)

        @pl.when(core_ref[0] != 0)
        def _():
            total = wide_ref[...]
            for value in ins[1:]:
                total = total + value[...].astype(f32)
            give[...], keep[...] = total[:half], total[half:]

    shape = (half, columns)
    return kernel(body, [(shape, f32)] * 2, [core, from_row], [wide, *parts])


def update_and_net(core, keep, got, own, chosen, taken):
    tokens, columns = own.shape

    def body(core_ref, keep_ref, got_ref, own_ref, chosen_ref, taken_ref, out):
        first = core_ref[0] == 0
        picked = jnp.where(first, keep_ref[...], got_ref[...])
        returned = jnp.where(first, got_ref[...], keep_ref[...])
        out[:tokens] = (chosen_ref[...] * (picked - own_ref[...])).astype(bf16)
        out[tokens:] = (returned - taken_ref[...]).astype(bf16)

    return kernel(
        body, [((2 * tokens, columns), bf16)], [core], [keep, got, own, chosen, taken]
    )[0]


def gradient_rows(core, cotangent, hidden, gathered, length):
    tokens, features = hidden.shape
    rows = features // (Y * CORES)
    columns = gathered[0][0].shape[1]
    half = tokens // STRETCHES

    def body(core_ref, cotangent_ref, hidden_ref, *refs):
        ins, out = refs[:-1], refs[-1]
        ins = [
            jnp.concatenate([value[...] for value in ins[at : at + TP]], axis=1)
            for at in range(0, TP * STRETCHES, TP)
        ]
        update = joined([value[:half] for value in ins], length)
        net = joined([value[half:] for value in ins], length)
        for y in range(Y):
            at = pl.ds(pl.multiple_of((y * CORES + core_ref[0]) * rows, rows), rows)
            block = dot(cotangent_ref[:, at], update, ((0,), (0,)))
            block = block + dot(hidden_ref[:, at], net, ((0,), (0,)))
            for k in range(TP):
                place = (k * Y + y) * rows
                out[place : place + rows] = block[:, k * columns : (k + 1) * columns]

    return kernel(
        body,
        [((TP * Y * rows, columns), f32)],
        [core],
        [cotangent, hidden, *sum(gathered, [])],
        flops=2 * tokens * features * columns * TP,
    )[0]


def intervention(core, hidden, gathered, own_block, near, far, length):
    tokens, features = hidden.shape
    half = features // 2
    count = TP * STRETCHES
    rows_each = tokens // STRETCHES

    def body(core_ref, hidden_ref, own_ref, *refs):
        ins, rest, out = refs[:count], refs[count:-1], refs[-1]
        ins = [
            jnp.concatenate([value[:rows_each] for value in ins[at : at + TP]], axis=1)
            for at in range(0, count, TP)
        ]
        update = joined(ins, length)
        for which, pieces in enumerate((rest[: TP - 1], rest[TP - 1 :])):
            place = core_ref[0] if which == 0 else 1 - core_ref[0]
            at = pl.ds(pl.multiple_of(place * half, half), half)
            rows = jnp.concatenate([own_ref[at]] + [value[...] for value in pieces], axis=1)
            added = dot(update, rows, ((1,), (1,)))
            out[:, at] = (hidden_ref[:, at].astype(f32) + added).astype(bf16)

    return kernel(
        body,
        [((tokens, features), bf16)],
        [core],
        [hidden, own_block, *sum(gathered, []), *near, *far],
        flops=2 * tokens * features * own_block.shape[1] * TP,
    )[0]


def per_device(hidden, cotangent, rotation, matching, mask):
    _, features = hidden.shape
    local_runs, length = mask.shape
    columns = rotation.shape[1]
    half = features // 2
    x, run_at = lax.axis_index("tp"), lax.axis_index("runs")
    z, y, core = run_at // 8, run_at // 2 % Y, run_at % CORES
    this_core, other_core = core[None], 1 - core[None]

    near = []
    for k in ORDER:
        start = (x + k) % TP * features + core * half
        part = lax.dynamic_slice(rotation, (start, 0), (half, columns)).astype(bf16)
        near.append(shift_tp(part, k))
    far = [swap_cores(value) for value in near]
    own_wide = lax.dynamic_slice(rotation, (x * features, 0), (features, columns))
    own_block, coords, pulled = own_products(hidden, cotangent, own_wide, length)

    own_runs = run_at * local_runs + jnp.arange(local_runs, dtype=jnp.int32)
    chosen = (mask * (matching != own_runs)[:, None].astype(jnp.int32)).astype(f32)
    chosen = jnp.broadcast_to(chosen[:, :, None], (local_runs, length, columns))
    each = length // STRETCHES
    chosen = [
        chosen[:, part * each : (part + 1) * each].reshape(local_runs * each, columns)
        for part in range(STRETCHES)
    ]

    chosen[0] = copied(chosen[0])

    matching, pulled[0] = lax.optimization_barrier((matching, pulled[0]))
    other_matching = swap_cores(matching)
    chip_match = jnp.concatenate(
        [
            jnp.where(core == 0, matching, other_matching),
            jnp.where(core == 0, other_matching, matching),
        ]
    )
    column_match = [shift_y(chip_match, -k) for k in range(Y)]

    chip_runs = local_runs * CORES

    def slots(match):
        return (z - match // (chip_runs * Y)) % Z * chip_runs + match % chip_runs

    asked = jnp.concatenate([slots(match) for match in column_match])
    targets = jnp.concatenate(
        [
            jnp.where(match // chip_runs % Y == y, slots(match), Z * chip_runs)
            for match in (column_match[-k % Y] for k in range(Y))
        ]
    )
    index = jnp.where(core == 0, asked, targets)
    from_row = (y - chip_match // chip_runs) % Y

    parts = partial_products(this_core, hidden, cotangent, near, far, length)
    for part in range(STRETCHES):
        parts[part] = [shift_tp(value, -k) for k, value in zip(ORDER, parts[part])]

    gathered = []
    for part in range(STRETCHES):
        own, taken, keep, give = summed(
            this_core, coords[part], pulled[part], parts[part], chosen[part]
        )
        first = both_cores(this_core, keep, swap_cores(give))
        line = [first] + ordered(lambda k: by_core(first, (k, 0), (0, k)))
        *routed, wide = route_runs(this_core, index, line, each)
        line = routed[:1] + ordered(lambda k: by_core(routed[k], (0, k), (-k, 0)))
        keep, give = finished_runs(this_core, from_row, wide, line, each)
        both = update_and_net(this_core, keep, swap_cores(give), own, chosen[part], taken)
        gathered.append([both] + ordered(lambda k: shift_tp(both, k)))
    near, far = ([value[ORDER.index(k)] for k in (1, 2, 3)] for value in (near, far))
    intervened = intervention(this_core, hidden, gathered, own_block, near, far, length)

    rows = features // (Y * CORES)
    away = gradient_rows(other_core, cotangent, hidden, gathered, length)
    grad = gradient_rows(this_core, cotangent, hidden, gathered, length) + swap_cores(away)
    grad = grad.astype(bf16).reshape(Z * Y, rows, columns)
    grad, intervened = lax.optimization_barrier((grad, intervened))
    groups = [[z * 8 + y * 2 + c for z in range(Z) for y in range(Y)] for c in range(CORES)]
    grad = lax.all_to_all(grad, "runs", 0, 0, axis_index_groups=groups, tiled=True)
    grad = jnp.sum(grad.astype(f32), axis=0)
    home = [
        ((z * 8 + y * 2 + c) * TP + x, (x * 8 + y * 2 + c) * TP + (x - z) % TP)
        for z in range(Z)
        for y in range(Y)
        for c in range(CORES)
        for x in range(TP)
    ]
    return intervened, lax.ppermute(grad, ("runs", "tp"), home)


def solution(mesh):
    def step(*arrays):
        return per_device(*arrays)

    in_specs = (P("runs", "tp"), P("runs", "tp"), P(None, "tp"), P("runs"), P("runs", None))
    out_specs = (P("runs", "tp"), P("runs", "tp"))
    step = jax.shard_map(
        step, mesh=mesh, in_specs=in_specs, out_specs=out_specs, check_vma=False
    )
    return step
```

```python
import jax
import jax.numpy as jnp
from jax import lax
from jax.experimental import pallas as pl
from jax.experimental.pallas import tpu as pltpu
from jax.sharding import PartitionSpec as P


Z, Y, CORES, TP = 4, 4, 2, 4
bf16, f32 = jnp.bfloat16, jnp.float32
ORDER = (1, 3, 2)
STRETCHES = 2
VMEM = pl.BlockSpec(memory_space=pltpu.VMEM)
SMEM = pl.BlockSpec(memory_space=pltpu.SMEM)


def along_runs(dz, dy, dcore):
    return [
        (z * 8 + y * 2 + c, (z + dz) % Z * 8 + (y + dy) % Y * 2 + (c + dcore) % CORES)
        for z in range(Z)
        for y in range(Y)
        for c in range(CORES)
    ]


def along_tp(dx):
    return [(x, (x + dx) % TP) for x in range(TP)]


def shift_tp(value, dx):
    return lax.ppermute(value, "tp", along_tp(dx)) if dx % TP else value


def shift_y(value, dy):
    return lax.ppermute(value, "runs", along_runs(0, dy, 0)) if dy % Y else value


def by_core(value, first, second):
    pairs = along_runs(*first, 0)[0::2] + along_runs(*second, 0)[1::2]
    return lax.ppermute(value, "runs", pairs)


def swap_cores(value):
    return lax.ppermute(value, "runs", along_runs(0, 0, 1))


def ordered(send):
    sent = {k: send(k) for k in ORDER}
    return [sent[k] for k in sorted(sent)]


def dot(a, b, dims=((1,), (0,))):
    return lax.dot_general(a, b, (dims, ((), ())), preferred_element_type=f32)


def kernel(body, outs, scalars, arrays, flops=0, scratch=(), grant=16):
    call = pl.pallas_call(
        body,
        out_shape=[jax.ShapeDtypeStruct(shape, dtype) for shape, dtype in outs],
        in_specs=[SMEM] * len(scalars) + [VMEM] * len(arrays),
        out_specs=[VMEM] * len(outs),
        scratch_shapes=list(scratch),
        compiler_params=pltpu.CompilerParams(vmem_limit_bytes=grant << 20),
        cost_estimate=pl.CostEstimate(flops=flops, bytes_accessed=0, transcendentals=0)
        if flops
        else None,
    )
    return call(*scalars, *arrays)


def stretched(value, length):
    each = length // STRETCHES
    starts = range(0, value.shape[0], length)
    return [
        jnp.concatenate([value[at + part * each : at + (part + 1) * each] for at in starts])
        for part in range(STRETCHES)
    ]


def joined(parts, length):
    each = length // STRETCHES
    starts = range(0, parts[0].shape[0], each)
    return jnp.concatenate([part[at : at + each] for at in starts for part in parts])


def own_products(hidden, cotangent, own, length):
    tokens = hidden.shape[0]
    shape = (tokens // STRETCHES, own.shape[1])

    def body(hidden_ref, cotangent_ref, own_ref, rounded, *outs):
        high = own_ref[...].astype(bf16)
        low = (own_ref[...] - high.astype(f32)).astype(bf16)
        rounded[...] = high
        both = jnp.concatenate([high, low], axis=1)
        for i, left in enumerate((hidden_ref, cotangent_ref)):
            total = dot(left[...], both)
            total = total[:, : shape[1]] + total[:, shape[1] :]
            for part, pieces in enumerate(stretched(total, length)):
                outs[i * STRETCHES + part][...] = pieces

    outs = kernel(
        body,
        [(own.shape, bf16)] + [(shape, f32)] * 2 * STRETCHES,
        [],
        [hidden, cotangent, own],
        flops=8 * tokens * own.shape[0] * own.shape[1],
    )
    return outs[0], list(outs[1 : 1 + STRETCHES]), list(outs[1 + STRETCHES :])


def partial_products(core, hidden, cotangent, near, far, length):
    tokens, features = hidden.shape
    half, columns = near[0].shape
    count = len(near)

    rows = 2 * tokens // STRETCHES

    def body(core_ref, hidden_ref, cotangent_ref, *refs):
        ins, outs = refs[: 2 * count], refs[2 * count :]
        at = pl.multiple_of(core_ref[0] * half, half)
        past = pl.multiple_of((1 - core_ref[0]) * half, half)
        here = jnp.concatenate([value[...] for value in ins[:count]], axis=1)
        there = jnp.concatenate([value[...] for value in ins[count:]], axis=1)
        for i, left in enumerate((hidden_ref, cotangent_ref)):
            total = dot(left[:, pl.ds(at, half)], here) + dot(left[:, pl.ds(past, half)], there)
            for part, pieces in enumerate(stretched(total.astype(bf16), length)):
                for k in range(count):
                    place = slice(i * rows // 2, (i + 1) * rows // 2)
                    outs[part * count + k][place] = pieces[:, k * columns : (k + 1) * columns]

    outs = kernel(
        body,
        [((rows, columns), bf16)] * count * STRETCHES,
        [core],
        [hidden, cotangent, *near, *far],
        flops=4 * tokens * features * columns * count,
    )
    return [outs[part * count : (part + 1) * count] for part in range(STRETCHES)]


def summed(core, coords, pulled, parts, chosen):
    tokens, columns = coords.shape

    def body(core_ref, coords_ref, pulled_ref, chosen_ref, *refs):
        ins, (own, taken, keep, give) = refs[: TP - 1], refs[TP - 1 :]
        total, other = coords_ref[...], pulled_ref[...]
        for value in ins:
            total = total + value[:tokens].astype(f32)
            other = other + value[tokens:].astype(f32)
        other = other * chosen_ref[...]
        own[...], taken[...] = total, other
        first = core_ref[0] == 0
        keep[...] = jnp.where(first, total, other).astype(bf16)
        give[...] = jnp.where(first, other, total).astype(bf16)

    shape = (tokens, columns)
    return kernel(
        body,
        [(shape, f32), (shape, f32), (shape, bf16), (shape, bf16)],
        [core],
        [coords, pulled, chosen, *parts],
    )


def laid_out(values):
    runs, length, columns = values[0].shape

    def body(*refs):
        for value, out in zip(refs[: len(values)], refs[len(values) :]):
            for i in range(runs):
                out[i * length : (i + 1) * length] = value[i]

    return kernel(body, [((runs * length, columns), f32)] * len(values), [], values)


def both_cores(core, keep, got):
    tokens, columns = keep.shape

    def body(core_ref, keep_ref, got_ref, out):
        out[pl.ds(pl.multiple_of(core_ref[0] * tokens, tokens), tokens)] = keep_ref[...]
        out[pl.ds(pl.multiple_of((1 - core_ref[0]) * tokens, tokens), tokens)] = got_ref[...]

    return kernel(body, [((2 * tokens, columns), bf16)], [core], [keep, got])[0]


def route_runs(core, index, parts, length):
    shape = parts[0].shape
    each = shape[0] // length
    slots = each * Z

    def body(core_ref, index_ref, *refs):
        ins, outs, (wide, packed, held) = refs[:Z], refs[Z : 2 * Z], refs[2 * Z :]

        @pl.when(core_ref[0] == 0)
        def _():
            for k, part in enumerate(ins):
                packed[k * shape[0] : (k + 1) * shape[0]] = part[...]
            for k, out in enumerate(outs):
                for i in range(each):
                    at = pl.multiple_of(index_ref[each * k + i] * length, length)
                    out[i * length : (i + 1) * length] = packed[pl.ds(at, length)]
            wide[...] = jnp.zeros_like(wide)

        @pl.when(core_ref[0] != 0)
        def _():
            held[...] = jnp.zeros_like(held)
            for k, part in enumerate(ins):
                for i in range(each):
                    at = pl.multiple_of(index_ref[each * k + i] * length, length)
                    at = pl.ds(at, length)
                    held[at] = held[at] + part[i * length : (i + 1) * length].astype(f32)
            for k, out in enumerate(outs):
                out[...] = held[k * shape[0] : (k + 1) * shape[0]].astype(bf16)
            wide[...] = held[: shape[0]]

    return kernel(
        body,
        [(shape, bf16)] * Z + [(shape, f32)],
        [core, index],
        parts,
        scratch=[
            pltpu.VMEM((slots * length, shape[1]), bf16),
            pltpu.VMEM(((slots + 1) * length, shape[1]), f32),
        ],
    )


def finished_runs(core, from_row, wide, parts, length):
    rows, columns = wide.shape
    half = rows // 2

    def body(core_ref, from_ref, wide_ref, *refs):
        ins, (keep, give) = refs[:Z], refs[Z:]

        @pl.when(core_ref[0] == 0)
        def _():
            for i in range(rows // length):
                at = slice(i * length, (i + 1) * length)
                source = from_ref[i]
                picked = ins[0][at]
                for k in range(1, Y):
                    picked = jnp.where(source == k, ins[k][at], picked)
                out = keep if i * length < half else give
                out[i * length % half : i * length % half + length] = picked.astype(f32)

        @pl.when(core_ref[0] != 0)
        def _():
            total = wide_ref[...]
            for value in ins[1:]:
                total = total + value[...].astype(f32)
            give[...], keep[...] = total[:half], total[half:]

    shape = (half, columns)
    return kernel(body, [(shape, f32)] * 2, [core, from_row], [wide, *parts])


def update_and_net(core, keep, got, own, chosen, taken):
    tokens, columns = own.shape

    def body(core_ref, keep_ref, got_ref, own_ref, chosen_ref, taken_ref, out):
        first = core_ref[0] == 0
        picked = jnp.where(first, keep_ref[...], got_ref[...])
        returned = jnp.where(first, got_ref[...], keep_ref[...])
        out[:tokens] = (chosen_ref[...] * (picked - own_ref[...])).astype(bf16)
        out[tokens:] = (returned - taken_ref[...]).astype(bf16)

    return kernel(
        body, [((2 * tokens, columns), bf16)], [core], [keep, got, own, chosen, taken]
    )[0]


def gradient_rows(core, cotangent, hidden, gathered, length):
    tokens, features = hidden.shape
    rows = features // (Y * CORES)
    columns = gathered[0][0].shape[1]
    half = tokens // STRETCHES

    def body(core_ref, cotangent_ref, hidden_ref, *refs):
        ins, out = refs[:-1], refs[-1]
        ins = [
            jnp.concatenate([value[...] for value in ins[at : at + TP]], axis=1)
            for at in range(0, TP * STRETCHES, TP)
        ]
        update = joined([value[:half] for value in ins], length)
        net = joined([value[half:] for value in ins], length)
        for y in range(Y):
            at = pl.ds(pl.multiple_of((y * CORES + core_ref[0]) * rows, rows), rows)
            block = dot(cotangent_ref[:, at], update, ((0,), (0,)))
            block = block + dot(hidden_ref[:, at], net, ((0,), (0,)))
            for k in range(TP):
                place = (k * Y + y) * rows
                out[place : place + rows] = block[:, k * columns : (k + 1) * columns]

    return kernel(
        body,
        [((TP * Y * rows, columns), f32)],
        [core],
        [cotangent, hidden, *sum(gathered, [])],
        flops=2 * tokens * features * columns * TP,
    )[0]


def intervention(core, hidden, gathered, own_block, near, far, length):
    tokens, features = hidden.shape
    half = features // 2
    count = TP * STRETCHES
    rows_each = tokens // STRETCHES

    def body(core_ref, hidden_ref, own_ref, *refs):
        ins, rest, out = refs[:count], refs[count:-1], refs[-1]
        ins = [
            jnp.concatenate([value[:rows_each] for value in ins[at : at + TP]], axis=1)
            for at in range(0, count, TP)
        ]
        update = joined(ins, length)
        for which, pieces in enumerate((rest[: TP - 1], rest[TP - 1 :])):
            place = core_ref[0] if which == 0 else 1 - core_ref[0]
            at = pl.ds(pl.multiple_of(place * half, half), half)
            rows = jnp.concatenate([own_ref[at]] + [value[...] for value in pieces], axis=1)
            added = dot(update, rows, ((1,), (1,)))
            out[:, at] = (hidden_ref[:, at].astype(f32) + added).astype(bf16)

    return kernel(
        body,
        [((tokens, features), bf16)],
        [core],
        [hidden, own_block, *sum(gathered, []), *near, *far],
        flops=2 * tokens * features * own_block.shape[1] * TP,
    )[0]


def per_device(hidden, cotangent, rotation, matching, mask):
    _, features = hidden.shape
    local_runs, length = mask.shape
    columns = rotation.shape[1]
    half = features // 2
    x, run_at = lax.axis_index("tp"), lax.axis_index("runs")
    z, y, core = run_at // 8, run_at // 2 % Y, run_at % CORES
    this_core, other_core = core[None], 1 - core[None]

    near = []
    for k in ORDER:
        start = (x + k) % TP * features + core * half
        part = lax.dynamic_slice(rotation, (start, 0), (half, columns)).astype(bf16)
        near.append(shift_tp(part, k))
    far = [swap_cores(value) for value in near]
    own_wide = lax.dynamic_slice(rotation, (x * features, 0), (features, columns))
    own_block, coords, pulled = own_products(hidden, cotangent, own_wide, length)

    own_runs = run_at * local_runs + jnp.arange(local_runs, dtype=jnp.int32)
    chosen = (mask * (matching != own_runs)[:, None].astype(jnp.int32)).astype(f32)
    chosen = jnp.broadcast_to(chosen[:, :, None], (local_runs, length, columns))
    each = length // STRETCHES
    chosen = [
        chosen[:, part * each : (part + 1) * each]
        for part in range(STRETCHES)
    ]

    chosen = laid_out(chosen)

    other_matching = swap_cores(matching)
    chip_match = jnp.concatenate(
        [
            jnp.where(core == 0, matching, other_matching),
            jnp.where(core == 0, other_matching, matching),
        ]
    )
    column_match = [shift_y(chip_match, -k) for k in range(Y)]

    chip_runs = local_runs * CORES

    def slots(match):
        return (z - match // (chip_runs * Y)) % Z * chip_runs + match % chip_runs

    asked = jnp.concatenate([slots(match) for match in column_match])
    targets = jnp.concatenate(
        [
            jnp.where(match // chip_runs % Y == y, slots(match), Z * chip_runs)
            for match in (column_match[-k % Y] for k in range(Y))
        ]
    )
    index = jnp.where(core == 0, asked, targets)
    from_row = (y - chip_match // chip_runs) % Y

    parts = partial_products(this_core, hidden, cotangent, near, far, length)
    for part in range(STRETCHES):
        parts[part] = [shift_tp(value, -k) for k, value in zip(ORDER, parts[part])]

    gathered = []
    for part in range(STRETCHES):
        own, taken, keep, give = summed(
            this_core, coords[part], pulled[part], parts[part], chosen[part]
        )
        first = both_cores(this_core, keep, swap_cores(give))
        line = [first] + ordered(lambda k: by_core(first, (k, 0), (0, k)))
        *routed, wide = route_runs(this_core, index, line, each)
        line = routed[:1] + ordered(lambda k: by_core(routed[k], (0, k), (-k, 0)))
        keep, give = finished_runs(this_core, from_row, wide, line, each)
        both = update_and_net(this_core, keep, swap_cores(give), own, chosen[part], taken)
        gathered.append([both] + ordered(lambda k: shift_tp(both, k)))
    near, far = ([value[ORDER.index(k)] for k in (1, 2, 3)] for value in (near, far))
    intervened = intervention(this_core, hidden, gathered, own_block, near, far, length)

    rows = features // (Y * CORES)
    away = gradient_rows(other_core, cotangent, hidden, gathered, length)
    grad = gradient_rows(this_core, cotangent, hidden, gathered, length) + swap_cores(away)
    grad = grad.astype(bf16).reshape(Z * Y, rows, columns)
    grad, intervened = lax.optimization_barrier((grad, intervened))
    groups = [[z * 8 + y * 2 + c for z in range(Z) for y in range(Y)] for c in range(CORES)]
    grad = lax.all_to_all(grad, "runs", 0, 0, axis_index_groups=groups, tiled=True)
    grad = jnp.sum(grad.astype(f32), axis=0)
    home = [
        ((z * 8 + y * 2 + c) * TP + x, (x * 8 + y * 2 + c) * TP + (x - z) % TP)
        for z in range(Z)
        for y in range(Y)
        for c in range(CORES)
        for x in range(TP)
    ]
    return intervened, lax.ppermute(grad, ("runs", "tp"), home)


def solution(mesh):
    def step(*arrays):
        return per_device(*arrays)

    in_specs = (P("runs", "tp"), P("runs", "tp"), P(None, "tp"), P("runs"), P("runs", None))
    out_specs = (P("runs", "tp"), P("runs", "tp"))
    step = jax.shard_map(
        step, mesh=mesh, in_specs=in_specs, out_specs=out_specs, check_vma=False
    )
    return step
```
